8 devices in a mesh: rep: 1 (over z), pp: 8 (over x, y, core).
Axes of the slice: x: 2, y: 2, z: 1, core: 2. Of those that a mesh axis runs over, the one named last changes fastest.
Arguments:
- x: bfloat16 [16, 512, 512], P('rep')
- dy: bfloat16 [16, 512, 512], P('rep')
- w_gate: bfloat16 [8, 512, 1792], P('pp')
- w_up: bfloat16 [8, 512, 1792], P('pp')
- w_down: bfloat16 [8, 1792, 512], P('pp')
Outputs:
- output 1: bfloat16 [8, 512, 1792], P(('rep', 'pp'))
- output 2: bfloat16 [8, 512, 1792], P(('rep', 'pp'))
- output 3: bfloat16 [8, 1792, 512], P(('rep', 'pp'))
All inputs are finite; a program needn't handle non-finite values.
Results may differ from the reference program's by a relative error of at most 0.029.
Values are sent between devices in bfloat16 or wider.
A program may use at most 2 GiB of HBM per device.

```python
import jax
import jax.numpy as jnp
from jax import lax

MICRO = 16
TOKENS = 512
D = 512
FF = 1792
LAYERS = 8
NAMES = ("w_gate", "w_up", "w_down")
SHAPES = {"w_gate": (LAYERS, D, FF), "w_up": (LAYERS, D, FF), "w_down": (LAYERS, FF, D)}


def bump(key, n, height):
    away = (jnp.arange(n, dtype=jnp.int32) - jax.random.randint(key, (), 0, n, jnp.int32)) % n
    return jnp.where(away < n // 8, height, 1.0)


def together(key, own, strength):
    shared = jax.random.normal(key, own.shape[1:], jnp.float32)
    return (own + strength * shared) * lax.rsqrt(1 + strength * strength)


def setup_inputs(seed: int = 0, part: int = 0) -> dict:
    kx, kdy, ka, kb, kz, kf, kh, kl, *kw = jax.random.split(jax.random.key(seed), 8 + len(NAMES))
    kx, kdy, ka, kb = (jax.random.fold_in(k, part) for k in (kx, kdy, ka, kb))
    shape = (MICRO, TOKENS, D)
    much_x, much_dy = jax.random.uniform(kz, (2,), jnp.float32, 0.0, 1.0)
    layers = 2.0 ** jax.random.uniform(kl, (LAYERS, 1, 1), jnp.float32, -1.0, 1.0)
    x = together(ka, jax.random.normal(kx, shape, jnp.float32), much_x) * bump(kf, D, 4.0)
    dy = together(kb, jax.random.normal(kdy, shape, jnp.float32), much_dy)
    drawn = {"x": x.astype(jnp.bfloat16), "dy": (dy * (MICRO * TOKENS) ** -0.5).astype(jnp.bfloat16)}
    for key, name in zip(kw, NAMES, strict=True):
        w = jax.random.normal(key, SHAPES[name], jnp.float32) * SHAPES[name][1] ** -0.5
        drawn[name] = (w * {"w_gate": 1.0, "w_up": bump(kh, FF, 4.0), "w_down": layers}[name]).astype(jnp.bfloat16)
    return drawn


def matmul(a, w):
    return jnp.dot(a, w, preferred_element_type=jnp.float32).astype(jnp.bfloat16)


def normed(h):
    wide = h.astype(jnp.float32)
    scale = lax.rsqrt(jnp.mean(wide**2, -1, keepdims=True) + 1e-6)
    return (wide * scale).astype(jnp.bfloat16)


def layer(h, w):
    a = normed(h)
    gate = jnp.dot(a, w["w_gate"], preferred_element_type=jnp.float32)
    up = jnp.dot(a, w["w_up"], preferred_element_type=jnp.float32)
    return h + matmul((jax.nn.silu(gate) * up).astype(jnp.bfloat16), w["w_down"])


def stack(weights, h):
    return lax.scan(lambda h, w: (layer(h, w), None), h, weights)[0]


def reference(x, dy, w_gate, w_up, w_down):
    weights = dict(zip(NAMES, (w_gate, w_up, w_down), strict=True))

    def take(so_far, one):
        h, by_y = one
        _, back = jax.vjp(lambda w: stack(w, h), weights)
        return jax.tree.map(lambda total, term: total + term.astype(jnp.float32), so_far, back(by_y)[0]), None

    none_yet = {name: jnp.zeros(w.shape, jnp.float32) for name, w in weights.items()}
    by_weights, _ = lax.scan(take, none_yet, (x, dy))
    return tuple(by_weights[name].astype(jnp.bfloat16) for name in NAMES)
```

```python
import functools

import jax
import jax.numpy as jnp
from jax import lax
from jax.experimental import pallas as pl
from jax.experimental.pallas import tpu as pltpu
from jax.sharding import PartitionSpec as P

BF, F32 = jnp.bfloat16, jnp.float32
LEAD = (12, 11, 10, 8, 6, 4, 2, 0)
LAG = (1, 2, 3, 4, 5, 6, 6, 6)
TILE = 256
PARTS = 2
NN = (((1,), (0,)), ((), ()))
NT = (((1,), (1,)), ((), ()))


def dot(a, b, dims=NN):
    return lax.dot_general(a, b, dims, preferred_element_type=F32)


def scaled(h):
    wide = h.astype(F32)
    return wide, lax.rsqrt(jnp.mean(wide * wide, -1, keepdims=True) + 1e-6)


def tiles(ff):
    return [pl.ds(n, TILE) for n in range(0, ff, TILE)]


def pick(me, values):
    out = jnp.int32(values[0])
    for i in range(1, len(values)):
        out = jnp.where(me == i, jnp.int32(values[i]), out)
    return out


def kernel(stages, x, dy, wg_in, wu_in, wd_in, og, ou, od, gu_all, s_all, *scratch):
    (hb, db, wg, wu, wd, acc, gu, gu_in, s_out, s_in, ys, dhs, at, dyt,
     h_sem, d_sem, y_sent, dh_sent, w_sem, gu_sem, gu_in_sem, s_sem, s_in_sem, o_sem) = scratch
    micro, tokens, _ = hb.shape
    ff = wg.shape[1]
    rows = tokens // PARTS
    last = stages - 1
    me = lax.axis_index("pp")
    lead, lag = pick(me, LEAD), pick(me, LAG)
    parts = [pl.ds(p * rows, rows) for p in range(PARTS)]

    weights = [pltpu.make_async_copy(a, b, w_sem.at[j]) for j, (a, b) in enumerate(((wg_in, wg), (wu_in, wu), (wd_in, wd)))]
    for copy in weights:
        copy.start()

    @pl.when(me == 0)
    def _():
        for m in range(micro):
            for p, r in enumerate(parts):
                pltpu.make_async_copy(x.at[m, r], hb.at[m, r], h_sem.at[m, p]).start()

    @pl.when(me == last)
    def _():
        for m in range(micro):
            for p, r in enumerate(parts):
                pltpu.make_async_copy(dy.at[m, r], db.at[m, r], d_sem.at[m, p]).start()

    barrier = pltpu.get_barrier_semaphore()

    @pl.when(me > 0)
    def _():
        pl.semaphore_signal(barrier, inc=1, device_id={"pp": me - 1}, device_id_type=pl.DeviceIdType.MESH)

    @pl.when(me < last)
    def _():
        pl.semaphore_signal(barrier, inc=1, device_id={"pp": me + 1}, device_id_type=pl.DeviceIdType.MESH)

    acc[...] = jnp.zeros_like(acc)

    pl.semaphore_wait(barrier, (me > 0).astype(jnp.int32) + (me < last).astype(jnp.int32))

    for copy in weights:
        copy.wait()

    def onward(m, p):
        r = parts[p]
        return pltpu.make_async_remote_copy(
            src_ref=ys.at[m % 2, r], dst_ref=hb.at[m, r], send_sem=y_sent.at[m % 2, p], recv_sem=h_sem.at[m, p],
            device_id={"pp": me + 1}, device_id_type=pl.DeviceIdType.MESH)

    def back_again(m, p):
        r = parts[p]
        return pltpu.make_async_remote_copy(
            src_ref=dhs.at[m % 2, r], dst_ref=db.at[m, r], send_sem=dh_sent.at[m % 2, p], recv_sem=d_sem.at[m, p],
            device_id={"pp": me - 1}, device_id_type=pl.DeviceIdType.MESH)

    def h_came(m, p):
        r = parts[p]
        return pltpu.make_async_copy(x.at[m, r], hb.at[m, r], h_sem.at[m, p])

    def d_came(m, p):
        r = parts[p]
        return pltpu.make_async_copy(dy.at[m, r], db.at[m, r], d_sem.at[m, p])

    def gu_out(m):
        return [pltpu.make_async_copy(gu.at[j], gu_all.at[m, j], gu_sem.at[j]) for j in range(2)]

    def gu_back(m):
        return [pltpu.make_async_copy(gu_all.at[m, j], gu_in.at[j], gu_in_sem.at[j]) for j in range(2)]

    def s_save(m):
        return [pltpu.make_async_copy(s_out.at[j], s_all.at[m, j], s_sem.at[j]) for j in range(3)]

    def s_back(m):
        return [pltpu.make_async_copy(s_all.at[m, j], s_in.at[j], s_in_sem.at[j]) for j in range(3)]

    def forward(m):
        for p, r in enumerate(parts):
            h_came(m, p).wait()
            h = hb[m, r, :]
            wide, scale = scaled(h)
            a = (wide * scale).astype(BF)
            for n in tiles(ff):
                g, u = dot(a, wg[:, n]), dot(a, wu[:, n])
                gu[0, r, n] = g
                gu[1, r, n] = u
                s_out[2, r, n] = (g * jax.nn.sigmoid(g) * u).astype(BF)
            y = dot(s_out[2, r, :], wd[...]).astype(BF)
            ys[m % 2, r, :] = h + y
            onward(m, p).start()

    def by_hidden(d, g, u, r, n):
        by_hid = dot(d, wd[n, :], NT).astype(BF).astype(F32)
        s = jax.nn.sigmoid(g)
        sg = g * s
        s_out[2, r, n] = (sg * u).astype(BF)
        s_out[1, r, n] = (sg * by_hid).astype(BF)
        s_out[0, r, n] = (by_hid * u * (s + sg * (1.0 - s))).astype(BF)

    def by_input(m, r, d):
        da = dot(s_out[0, r, :], wg[...], NT).astype(BF) + dot(s_out[1, r, :], wu[...], NT).astype(BF)
        wide, scale = scaled(hb[m, r, :])
        da = da.astype(F32)
        c = jnp.sum(wide * da, -1, keepdims=True) * (scale * scale * scale) * (1.0 / hb.shape[2])
        dhs[m % 2, r, :] = d + (da * scale - wide * c).astype(BF)

    def backward(m):
        @pl.when(me == last)
        def _():
            for p, r in enumerate(parts):
                h_came(m, p).wait()
                d_came(m, p).wait()
                wide, scale = scaled(hb[m, r, :])
                a = (wide * scale).astype(BF)
                d = db[m, r, :]
                for n in tiles(ff):
                    by_hidden(d, dot(a, wg[:, n]), dot(a, wu[:, n]), r, n)
                by_input(m, r, d)
                back_again(m, p).start()

        @pl.when((me > 0) & (me < last))
        def _():
            for copy in gu_back(m):
                copy.wait()
            for p, r in enumerate(parts):
                d_came(m, p).wait()
                d = db[m, r, :]
                for n in tiles(ff):
                    by_hidden(d, gu_in[0, r, n], gu_in[1, r, n], r, n)
                by_input(m, r, d)
                back_again(m, p).start()

        @pl.when(me == 0)
        def _():
            for copy in gu_back(m):
                copy.wait()
            for p, r in enumerate(parts):
                d_came(m, p).wait()
                d = db[m, r, :]
                for n in tiles(ff):
                    by_hidden(d, gu_in[0, r, n], gu_in[1, r, n], r, n)

    def by_weights(m):
        for copy in s_back(m):
            copy.wait()
        wide, scale = scaled(hb[m])
        at[...] = (wide * scale).astype(BF).T
        dyt[...] = db[m].T
        for j, left in enumerate((at, at, dyt)):
            for n in tiles(ff):
                acc[j, :, n] += dot(left[...], s_in[j, :, n]).astype(BF).astype(F32)

    def step(t, carry):
        mb, mw = t - lead, t - lead - lag
        has_f = (me < last) & (t < micro)
        has_b = (mb >= 0) & (mb < micro)
        has_w = (mw >= 0) & (mw < micro)

        @pl.when((me < last) & (t >= 1) & (t <= micro))
        def _():
            for copy in gu_out(t - 1):
                copy.wait()

        @pl.when((mb >= 1) & (mb <= micro))
        def _():
            for copy in s_save(mb - 1):
                copy.wait()

        @pl.when(has_b & (me < last))
        def _():
            for copy in gu_back(mb):
                copy.start()

        @pl.when(has_w)
        def _():
            for copy in s_back(mw):
                copy.start()

        @pl.when(has_f & (t >= 2))
        def _():
            for p in range(PARTS):
                onward(t - 2, p).wait_send()

        @pl.when(has_f)
        def _():
            forward(t)
            for copy in gu_out(t):
                copy.start()

        @pl.when(has_b & (me > 0) & (mb >= 2))
        def _():
            for p in range(PARTS):
                back_again(mb - 2, p).wait_send()

        @pl.when(has_b)
        def _():
            backward(mb)
            for copy in s_save(mb):
                copy.start()

        @pl.when(has_w)
        def _():
            by_weights(mw)

        return carry

    lax.fori_loop(0, micro + lead + lag, step, 0)

    out = [pltpu.make_async_copy(s_in.at[j], o, o_sem.at[j]) for j, o in enumerate((og, ou, od))]
    for j in range(3):
        s_in[j] = acc[j].astype(BF)
        out[j].start()

    @pl.when(me < last)
    def _():
        for m in (micro - 2, micro - 1):
            for p in range(PARTS):
                onward(m, p).wait_send()

    @pl.when(me > 0)
    def _():
        for m in (micro - 2, micro - 1):
            for p in range(PARTS):
                back_again(m, p).wait_send()

    for copy in out:
        copy.wait()


def solution(mesh):
    stages = mesh.shape["pp"]

    def step(x, dy, wg, wu, wd):
        micro, tokens, d = x.shape
        ff = wg.shape[2]
        vmem, dma = pltpu.VMEM, pltpu.SemaphoreType.DMA
        wide = jax.ShapeDtypeStruct((d, ff), BF)
        og, ou, od, _, _ = pl.pallas_call(
            functools.partial(kernel, stages),
            out_shape=(wide, wide, wide,
                       jax.ShapeDtypeStruct((micro, 2, tokens, ff), F32), jax.ShapeDtypeStruct((micro, 3, tokens, ff), BF)),
            in_specs=[pl.BlockSpec(memory_space=pl.ANY)] * 5,
            out_specs=[pl.BlockSpec(memory_space=pl.ANY)] * 5,
            scratch_shapes=[
                vmem((micro, tokens, d), BF), vmem((micro, tokens, d), BF),
                vmem((d, ff), BF), vmem((d, ff), BF), vmem((ff, d), BF),
                vmem((3, d, ff), F32),
                vmem((2, tokens, ff), F32), vmem((2, tokens, ff), F32),
                vmem((3, tokens, ff), BF), vmem((3, tokens, ff), BF),
                vmem((2, tokens, d), BF), vmem((2, tokens, d), BF),
                vmem((d, tokens), BF), vmem((d, tokens), BF),
                dma((micro, PARTS)), dma((micro, PARTS)), dma((2, PARTS)), dma((2, PARTS)),
                dma((3,)), dma((2,)), dma((2,)), dma((3,)), dma((3,)), dma((3,)),
            ],
            compiler_params=pltpu.CompilerParams(collective_id=0, has_side_effects=True, vmem_limit_bytes=67043328),
            name="pipeline",
        )(x, dy, wg[0], wu[0], wd[0])
        return og[None], ou[None], od.T[None]

    return jax.shard_map(
        step,
        mesh=mesh,
        in_specs=(P("rep", None, None),) * 2 + (P("pp", None, None),) * 3,
        out_specs=(P(("rep", "pp"), None, None),) * 3,
        check_vma=False,
    )
```

```python
import functools

import jax
import jax.numpy as jnp
from jax import lax
from jax.experimental import pallas as pl
from jax.experimental.pallas import tpu as pltpu
from jax.sharding import PartitionSpec as P

BF, F32 = jnp.bfloat16, jnp.float32
LEAD = (15, 13, 11, 10, 6, 5, 2, 0)
LAG = (2, 3, 5, 6, 9, 10, 10, 5)
VIA = range(3, 13)
VIA_SLOTS = 6
TILE = 256
PARTS = 2
NN = (((1,), (0,)), ((), ()))
NT = (((1,), (1,)), ((), ()))


def dot(a, b, dims=NN):
    return lax.dot_general(a, b, dims, preferred_element_type=F32)


def scaled(h):
    wide = h.astype(F32)
    return wide, lax.rsqrt(jnp.mean(wide * wide, -1, keepdims=True) + 1e-6)


def tiles(ff):
    return [pl.ds(n, TILE) for n in range(0, ff, TILE)]


def pick(me, values):
    out = jnp.int32(values[0])
    for i in range(1, len(values)):
        out = jnp.where(me == i, jnp.int32(values[i]), out)
    return out


def kernel(stages, x, dy, wg_in, wu_in, wd_in, og, ou, od, gu_all, s_all, *scratch):
    (hb, db, wg, wu, wd, acc, gu, gu_in, s_out, s_in, hid, via, ys, dhs, at, dyt,
     h_sem, d_sem, y_sent, dh_sent, w_sem, gu_sem, gu_in_sem, s_sem, s_in_sem, o_sem, via_sem, via_sent) = scratch
    micro, tokens, _ = hb.shape
    ff = wg.shape[1]
    rows = tokens // PARTS
    last = stages - 1
    me = lax.axis_index("pp")
    lead, lag = pick(me, LEAD), pick(me, LAG)
    parts = [pl.ds(p * rows, rows) for p in range(PARTS)]

    weights = [pltpu.make_async_copy(a, b, w_sem.at[j]) for j, (a, b) in enumerate(((wg_in, wg), (wu_in, wu), (wd_in, wd)))]
    for copy in weights:
        copy.start()

    @pl.when(me == 0)
    def _():
        for m in range(micro):
            for p, r in enumerate(parts):
                pltpu.make_async_copy(x.at[m, r], hb.at[m, r], h_sem.at[m, p]).start()

    @pl.when(me == last)
    def _():
        for m in range(micro):
            for p, r in enumerate(parts):
                pltpu.make_async_copy(dy.at[m, r], db.at[m, r], d_sem.at[m, p]).start()

    low, high = stages // 2 - 1, stages // 2
    peers = [(i, i + 1) for i in range(last)] + [(a, b) for a in (0, last) for b in (low, high)]
    barrier = pltpu.get_barrier_semaphore()
    for a, b in peers:
        for one, other in ((a, b), (b, a)):
            @pl.when(me == one)
            def _():
                pl.semaphore_signal(barrier, inc=1, device_id={"pp": other}, device_id_type=pl.DeviceIdType.MESH)

    acc[...] = jnp.zeros_like(acc)

    pl.semaphore_wait(barrier, pick(me, [sum(i in pair for pair in peers) for i in range(stages)]))

    for copy in weights:
        copy.wait()

    def onward(m, p):
        r = parts[p]
        return pltpu.make_async_remote_copy(
            src_ref=ys.at[m % 2, r], dst_ref=hb.at[m, r], send_sem=y_sent.at[m % 2, p], recv_sem=h_sem.at[m, p],
            device_id={"pp": me + 1}, device_id_type=pl.DeviceIdType.MESH)

    def back_again(m, p):
        r = parts[p]
        return pltpu.make_async_remote_copy(
            src_ref=dhs.at[m % 2, r], dst_ref=db.at[m, r], send_sem=dh_sent.at[m % 2, p], recv_sem=d_sem.at[m, p],
            device_id={"pp": me - 1}, device_id_type=pl.DeviceIdType.MESH)

    def remote(src, dst, sent, came, device):
        return pltpu.make_async_remote_copy(src_ref=src, dst_ref=dst, send_sem=sent, recv_sem=came,
                                            device_id={"pp": device}, device_id_type=pl.DeviceIdType.MESH)

    half = PARTS - 1

    def goes_via(m):
        return (m >= VIA.start) & (m < VIA.stop)

    def onward_via(m):
        return remote(ys.at[m % 2, parts[half]], via.at[m % VIA_SLOTS], y_sent.at[m % 2, half], via_sem.at[m % VIA_SLOTS], 0)

    def back_via(m):
        return remote(dhs.at[m % 2, parts[half]], via.at[m % VIA_SLOTS], dh_sent.at[m % 2, half], via_sem.at[m % VIA_SLOTS], last)

    def pass_onward(m):
        return remote(via.at[m % VIA_SLOTS], hb.at[m, parts[half]], via_sent, h_sem.at[m, half], high)

    def pass_back(m):
        return remote(via.at[m % VIA_SLOTS], db.at[m, parts[half]], via_sent, d_sem.at[m, half], low)

    def send(direct, indirect, m, p, at_stage):
        if p < half:
            direct(m, p).start()
            return
        other_way = (me == at_stage) & goes_via(m)

        @pl.when(other_way)
        def _():
            indirect(m).start()

        @pl.when(jnp.logical_not(other_way))
        def _():
            direct(m, p).start()

    def h_came(m, p):
        r = parts[p]
        return pltpu.make_async_copy(x.at[m, r], hb.at[m, r], h_sem.at[m, p])

    def d_came(m, p):
        r = parts[p]
        return pltpu.make_async_copy(dy.at[m, r], db.at[m, r], d_sem.at[m, p])

    def gu_out(m, p):
        return pltpu.make_async_copy(gu.at[:, parts[p]], gu_all.at[m, :, parts[p]], gu_sem.at[p])

    def gu_back(m, p):
        return pltpu.make_async_copy(gu_all.at[m, :, parts[p]], gu_in.at[:, parts[p]], gu_in_sem.at[p])

    def s_save(m, p):
        return pltpu.make_async_copy(s_out.at[:, parts[p]], s_all.at[m, :, parts[p]], s_sem.at[p])

    def s_back(m, j):
        return pltpu.make_async_copy(s_all.at[m, j], s_in.at[j], s_in_sem.at[j])

    def forward(m):
        @pl.when(m >= 1)
        def _():
            for p in range(PARTS):
                gu_out(m - 1, p).wait()

        @pl.when(m >= 2)
        def _():
            for p in range(PARTS):
                onward(m - 2, p).wait_send()

        for p, r in enumerate(parts):
            h_came(m, p).wait()
            h = hb[m, r, :]
            wide, scale = scaled(h)
            a = (wide * scale).astype(BF)
            for n in tiles(ff):
                g, u = dot(a, wg[:, n]), dot(a, wu[:, n])
                gu[0, r, n] = g
                gu[1, r, n] = u
                hid[p % 2, :, n] = (g * jax.nn.sigmoid(g) * u).astype(BF)
            y = dot(hid[p % 2], wd[...]).astype(BF)
            ys[m % 2, r, :] = h + y
            send(onward, onward_via, m, p, low)
            gu_out(m, p).start()

    def by_hidden(d, g, u, r, n):
        by_hid = dot(d, wd[n, :], NT).astype(BF).astype(F32)
        s = jax.nn.sigmoid(g)
        sg = g * s
        s_out[2, r, n] = (sg * u).astype(BF)
        s_out[1, r, n] = (sg * by_hid).astype(BF)
        s_out[0, r, n] = (by_hid * u * (s + sg * (1.0 - s))).astype(BF)

    def by_input(m, r, d):
        da = dot(s_out[0, r, :], wg[...], NT).astype(BF) + dot(s_out[1, r, :], wu[...], NT).astype(BF)
        wide, scale = scaled(hb[m, r, :])
        da = da.astype(F32)
        c = jnp.sum(wide * da, -1, keepdims=True) * (scale * scale * scale) * (1.0 / hb.shape[2])
        dhs[m % 2, r, :] = d + (da * scale - wide * c).astype(BF)

    def backward_part(m, p, first, final):
        r = parts[p]
        d_came(m, p).wait()
        d = db[m, r, :]
        if final:
            h_came(m, p).wait()
            wide, scale = scaled(hb[m, r, :])
            a = (wide * scale).astype(BF)
            for n in tiles(ff):
                by_hidden(d, dot(a, wg[:, n]), dot(a, wu[:, n]), r, n)
        else:
            gu_back(m, p).wait()
            for n in tiles(ff):
                by_hidden(d, gu_in[0, r, n], gu_in[1, r, n], r, n)
        if not first:
            by_input(m, r, d)
            send(back_again, back_via, m, p, high)
        s_save(m, p).start()
        if not final:
            gu_back(jnp.minimum(m + 1, micro - 1), p).start()

    def backward(m):
        for first, final, here in ((True, False, me == 0), (False, False, (me > 0) & (me < last)), (False, True, me == last)):
            @pl.when(here)
            def _():
                @pl.when(m >= 1)
                def _():
                    for p in range(PARTS):
                        s_save(m - 1, p).wait()

                if not first:
                    @pl.when(m >= 2)
                    def _():
                        for p in range(PARTS):
                            back_again(m - 2, p).wait_send()

                for p in range(PARTS):
                    backward_part(m, p, first, final)

    def by_weights(m):
        for j in range(3):
            s_back(m, j).wait()
        dyt[...] = db[m].T
        wide, scale = scaled(hb[m])
        at[...] = (wide * scale).astype(BF).T
        for j, left in ((2, dyt), (0, at), (1, at)):
            for n in tiles(ff):
                acc[j, :, n] += dot(left[...], s_in[j, :, n]).astype(BF).astype(F32)
        for j in range(3):
            s_back(jnp.minimum(m + 1, micro - 1), j).start()

    def step(t, carry):
        mb, mw = t - lead, t - lead - lag
        passed = t - VIA_SLOTS

        @pl.when((me == 0) & goes_via(passed))
        def _():
            pass_onward(passed).wait_send()

        @pl.when((me == last) & goes_via(passed))
        def _():
            pass_back(passed).wait_send()

        @pl.when((me == 0) & goes_via(passed + 1))
        def _():
            onward_via(passed + 1).wait_recv()
            pass_onward(passed + 1).start()

        @pl.when((me == last) & goes_via(passed + 1))
        def _():
            back_via(passed + 1).wait_recv()
            pass_back(passed + 1).start()

        @pl.when((me < last) & (t == micro))
        def _():
            for p in range(PARTS):
                gu_out(micro - 1, p).wait()

        @pl.when(mb == micro)
        def _():
            for p in range(PARTS):
                s_save(micro - 1, p).wait()

        @pl.when((me < last) & (mb == micro))
        def _():
            for p in range(PARTS):
                gu_back(micro - 1, p).wait()

        @pl.when((me < last) & (mb == 0))
        def _():
            for p in range(PARTS):
                gu_back(0, p).start()

        @pl.when(mw == 0)
        def _():
            for j in range(3):
                s_back(0, j).start()

        @pl.when((me < last) & (t < micro))
        def _():
            forward(t)

        @pl.when((mb >= 0) & (mb < micro))
        def _():
            backward(mb)

        @pl.when((mw >= 0) & (mw < micro))
        def _():
            by_weights(mw)

        return carry

    lax.fori_loop(0, micro + lead + lag, step, 0)

    for j in range(3):
        s_back(micro - 1, j).wait()

    out = [pltpu.make_async_copy(s_in.at[j], o, o_sem.at[j]) for j, o in enumerate((og, ou, od))]
    for j in range(3):
        s_in[j] = acc[j].astype(BF)
        out[j].start()

    @pl.when(me < last)
    def _():
        for m in (micro - 2, micro - 1):
            for p in range(PARTS):
                onward(m, p).wait_send()

    @pl.when(me > 0)
    def _():
        for m in (micro - 2, micro - 1):
            for p in range(PARTS):
                back_again(m, p).wait_send()

    for copy in out:
        copy.wait()


def solution(mesh):
    stages = mesh.shape["pp"]

    def step(x, dy, wg, wu, wd):
        micro, tokens, d = x.shape
        ff = wg.shape[2]
        vmem, dma = pltpu.VMEM, pltpu.SemaphoreType.DMA
        wide = jax.ShapeDtypeStruct((d, ff), BF)
        og, ou, od, _, _ = pl.pallas_call(
            functools.partial(kernel, stages),
            out_shape=(wide, wide, wide,
                       jax.ShapeDtypeStruct((micro, 2, tokens, ff), F32), jax.ShapeDtypeStruct((micro, 3, tokens, ff), BF)),
            in_specs=[pl.BlockSpec(memory_space=pl.ANY)] * 5,
            out_specs=[pl.BlockSpec(memory_space=pl.ANY)] * 5,
            scratch_shapes=[
                vmem((micro, tokens, d), BF), vmem((micro, tokens, d), BF),
                vmem((d, ff), BF), vmem((d, ff), BF), vmem((ff, d), BF),
                vmem((3, d, ff), F32),
                vmem((2, tokens, ff), F32), vmem((2, tokens, ff), F32),
                vmem((3, tokens, ff), BF), vmem((3, tokens, ff), BF), vmem((2, tokens // PARTS, ff), BF), vmem((VIA_SLOTS, tokens // PARTS, d), BF),
                vmem((2, tokens, d), BF), vmem((2, tokens, d), BF),
                vmem((d, tokens), BF), vmem((d, tokens), BF),
                dma((micro, PARTS)), dma((micro, PARTS)), dma((2, PARTS)), dma((2, PARTS)),
                dma((3,)), dma((PARTS,)), dma((PARTS,)), dma((PARTS,)), dma((3,)), dma((3,)), dma((VIA_SLOTS,)), dma,
            ],
            compiler_params=pltpu.CompilerParams(collective_id=0, has_side_effects=True, vmem_limit_bytes=67043328),
            name="pipeline",
        )(x, dy, wg[0], wu[0], wd[0])
        return og[None], ou[None], od.T[None]

    return jax.shard_map(
        step,
        mesh=mesh,
        in_specs=(P("rep", None, None),) * 2 + (P("pp", None, None),) * 3,
        out_specs=(P(("rep", "pp"), None, None),) * 3,
        check_vma=False,
    )
```

```python
import functools

import jax
import jax.numpy as jnp
from jax import lax
from jax.experimental import pallas as pl
from jax.experimental.pallas import tpu as pltpu
from jax.sharding import PartitionSpec as P

BF, F32 = jnp.bfloat16, jnp.float32
LEAD = (14, 13, 11, 10, 6, 5, 2, 0)
LAG = (2, 3, 5, 6, 9, 10, 11, 6)
VIA = range(3, 13)
VIA_SLOTS = 6
TILE = 256
PARTS = 2
NN = (((1,), (0,)), ((), ()))
NT = (((1,), (1,)), ((), ()))


def dot(a, b, dims=NN):
    return lax.dot_general(a, b, dims, preferred_element_type=F32)


def scaled(h):
    wide = h.astype(F32)
    return wide, lax.rsqrt(jnp.mean(wide * wide, -1, keepdims=True) + 1e-6)


def tiles(ff):
    return [pl.ds(n, TILE) for n in range(0, ff, TILE)]


def pick(me, values):
    out = jnp.int32(values[0])
    for i in range(1, len(values)):
        out = jnp.where(me == i, jnp.int32(values[i]), out)
    return out


def kernel(stages, x, dy, wg_in, wu_in, wd_in, og, ou, od, gu_all, s_all, *scratch):
    (hb, db, wg, wu, wd, acc, gu, gu_in, s_out, s_in, hid, via, ys, dhs, at, dyt,
     h_sem, d_sem, y_sent, dh_sent, w_sem, gu_sem, gu_in_sem, s_sem, s_in_sem, o_sem, via_sem, via_sent) = scratch
    micro, tokens, _ = hb.shape
    ff = wg.shape[1]
    rows = tokens // PARTS
    last = stages - 1
    me = lax.axis_index("pp")
    lead, lag = pick(me, LEAD), pick(me, LAG)
    parts = [pl.ds(p * rows, rows) for p in range(PARTS)]

    weights = [pltpu.make_async_copy(a, b, w_sem.at[j]) for j, (a, b) in enumerate(((wg_in, wg), (wu_in, wu), (wd_in, wd)))]
    for copy in weights:
        copy.start()

    @pl.when(me == 0)
    def _():
        for m in range(micro):
            for p, r in enumerate(parts):
                pltpu.make_async_copy(x.at[m, r], hb.at[m, r], h_sem.at[m, p]).start()

    @pl.when(me == last)
    def _():
        for m in range(micro):
            for p, r in enumerate(parts):
                pltpu.make_async_copy(dy.at[m, r], db.at[m, r], d_sem.at[m, p]).start()

    low, high = stages // 2 - 1, stages // 2
    peers = [(i, i + 1) for i in range(last)] + [(a, b) for a in (0, last) for b in (low, high)]
    barrier = pltpu.get_barrier_semaphore()
    for a, b in peers:
        for one, other in ((a, b), (b, a)):
            @pl.when(me == one)
            def _():
                pl.semaphore_signal(barrier, inc=1, device_id={"pp": other}, device_id_type=pl.DeviceIdType.MESH)

    acc[...] = jnp.zeros_like(acc)

    pl.semaphore_wait(barrier, pick(me, [sum(i in pair for pair in peers) for i in range(stages)]))

    for copy in weights:
        copy.wait()

    def onward(m, p):
        r = parts[p]
        return pltpu.make_async_remote_copy(
            src_ref=ys.at[m % 2, r], dst_ref=hb.at[m, r], send_sem=y_sent.at[m % 2, p], recv_sem=h_sem.at[m, p],
            device_id={"pp": me + 1}, device_id_type=pl.DeviceIdType.MESH)

    def back_again(m, p):
        r = parts[p]
        return pltpu.make_async_remote_copy(
            src_ref=dhs.at[m % 2, r], dst_ref=db.at[m, r], send_sem=dh_sent.at[m % 2, p], recv_sem=d_sem.at[m, p],
            device_id={"pp": me - 1}, device_id_type=pl.DeviceIdType.MESH)

    def remote(src, dst, sent, came, device):
        return pltpu.make_async_remote_copy(src_ref=src, dst_ref=dst, send_sem=sent, recv_sem=came,
                                            device_id={"pp": device}, device_id_type=pl.DeviceIdType.MESH)

    half = PARTS - 1

    def goes_via(m):
        return (m >= VIA.start) & (m < VIA.stop)

    def onward_via(m):
        return remote(ys.at[m % 2, parts[half]], via.at[m % VIA_SLOTS], y_sent.at[m % 2, half], via_sem.at[m % VIA_SLOTS], 0)

    def back_via(m):
        return remote(dhs.at[m % 2, parts[half]], via.at[m % VIA_SLOTS], dh_sent.at[m % 2, half], via_sem.at[m % VIA_SLOTS], last)

    def pass_onward(m):
        return remote(via.at[m % VIA_SLOTS], hb.at[m, parts[half]], via_sent, h_sem.at[m, half], high)

    def pass_back(m):
        return remote(via.at[m % VIA_SLOTS], db.at[m, parts[half]], via_sent, d_sem.at[m, half], low)

    def send(direct, indirect, m, p, at_stage):
        if p < half:
            direct(m, p).start()
            return
        other_way = (me == at_stage) & goes_via(m)

        @pl.when(other_way)
        def _():
            indirect(m).start()

        @pl.when(jnp.logical_not(other_way))
        def _():
            direct(m, p).start()

    def h_came(m, p):
        r = parts[p]
        return pltpu.make_async_copy(x.at[m, r], hb.at[m, r], h_sem.at[m, p])

    def d_came(m, p):
        r = parts[p]
        return pltpu.make_async_copy(dy.at[m, r], db.at[m, r], d_sem.at[m, p])

    def gu_out(m, p):
        return pltpu.make_async_copy(gu.at[:, parts[p]], gu_all.at[m, :, parts[p]], gu_sem.at[p])

    def gu_back(m, p):
        return pltpu.make_async_copy(gu_all.at[m, :, parts[p]], gu_in.at[:, parts[p]], gu_in_sem.at[p])

    def s_save(m, p):
        return pltpu.make_async_copy(s_out.at[:, parts[p]], s_all.at[m, :, parts[p]], s_sem.at[p])

    def s_back(m, j):
        return pltpu.make_async_copy(s_all.at[m, j], s_in.at[j], s_in_sem.at[j])

    def forward(m):
        @pl.when(m >= 2)
        def _():
            for p in range(PARTS):
                onward(m - 2, p).wait_send()

        for p, r in enumerate(parts):
            h_came(m, p).wait()
            h = hb[m, r, :]
            wide, scale = scaled(h)
            a = (wide * scale).astype(BF)
            for n in tiles(ff):
                g, u = dot(a, wg[:, n]), dot(a, wu[:, n])
                gu[0, r, n] = g
                gu[1, r, n] = u
                hid[p % 2, :, n] = (g * jax.nn.sigmoid(g) * u).astype(BF)
            y = dot(hid[p % 2], wd[...]).astype(BF)
            ys[m % 2, r, :] = h + y
            send(onward, onward_via, m, p, low)
            gu_out(m, p).start()

    def by_hidden(d, g, u, r, n):
        by_hid = dot(d, wd[n, :], NT).astype(BF).astype(F32)
        s = jax.nn.sigmoid(g)
        sg = g * s
        s_out[2, r, n] = (sg * u).astype(BF)
        s_out[1, r, n] = (sg * by_hid).astype(BF)
        s_out[0, r, n] = (by_hid * u * (s + sg * (1.0 - s))).astype(BF)

    def by_input(m, r, d):
        da = dot(s_out[0, r, :], wg[...], NT).astype(BF) + dot(s_out[1, r, :], wu[...], NT).astype(BF)
        wide, scale = scaled(hb[m, r, :])
        da = da.astype(F32)
        c = jnp.sum(wide * da, -1, keepdims=True) * (scale * scale * scale) * (1.0 / hb.shape[2])
        dhs[m % 2, r, :] = d + (da * scale - wide * c).astype(BF)

    def backward_part(m, p, first, final):
        r = parts[p]
        d_came(m, p).wait()
        d = db[m, r, :]
        if final:
            h_came(m, p).wait()
            wide, scale = scaled(hb[m, r, :])
            a = (wide * scale).astype(BF)
            for n in tiles(ff):
                by_hidden(d, dot(a, wg[:, n]), dot(a, wu[:, n]), r, n)
        else:
            gu_back(m, p).wait()
            for n in tiles(ff):
                by_hidden(d, gu_in[0, r, n], gu_in[1, r, n], r, n)
        if not first:
            by_input(m, r, d)
            send(back_again, back_via, m, p, high)
        s_save(m, p).start()
        if not final:
            gu_back(jnp.minimum(m + 1, micro - 1), p).start()

    def backward(m):
        for first, final, here in ((True, False, me == 0), (False, False, (me > 0) & (me < last)), (False, True, me == last)):
            @pl.when(here)
            def _():
                @pl.when(m >= 1)
                def _():
                    for p in range(PARTS):
                        s_save(m - 1, p).wait()

                if not first:
                    @pl.when(m >= 2)
                    def _():
                        for p in range(PARTS):
                            back_again(m - 2, p).wait_send()

                for p in range(PARTS):
                    backward_part(m, p, first, final)

    def by_weights(m):
        for j in range(3):
            s_back(m, j).wait()
        dyt[...] = db[m].T
        wide, scale = scaled(hb[m])
        at[...] = (wide * scale).astype(BF).T
        for j, left in ((2, dyt), (0, at), (1, at)):
            for n in tiles(ff):
                acc[j, :, n] += dot(left[...], s_in[j, :, n]).astype(BF).astype(F32)
        for j in range(3):
            s_back(jnp.minimum(m + 1, micro - 1), j).start()

    def step(t, carry):
        mb, mw = t - lead, t - lead - lag
        passed = t - VIA_SLOTS

        @pl.when((me == 0) & goes_via(passed))
        def _():
            pass_onward(passed).wait_send()

        @pl.when((me == last) & goes_via(passed))
        def _():
            pass_back(passed).wait_send()

        @pl.when((me == 0) & goes_via(passed + 1))
        def _():
            onward_via(passed + 1).wait_recv()
            pass_onward(passed + 1).start()

        @pl.when((me == last) & goes_via(passed + 1))
        def _():
            back_via(passed + 1).wait_recv()
            pass_back(passed + 1).start()

        @pl.when((me < last) & (t >= 1) & (t <= micro))
        def _():
            for p in range(PARTS):
                gu_out(t - 1, p).wait()

        @pl.when(mb == micro)
        def _():
            for p in range(PARTS):
                s_save(micro - 1, p).wait()

        @pl.when((me < last) & (mb == micro))
        def _():
            for p in range(PARTS):
                gu_back(micro - 1, p).wait()

        @pl.when((me < last) & (mb == -1))
        def _():
            for p in range(PARTS):
                gu_back(0, p).start()

        @pl.when(mw == 0)
        def _():
            for j in range(3):
                s_back(0, j).start()

        @pl.when((mb >= 0) & (mb < micro))
        def _():
            backward(mb)

        @pl.when((me < last) & (t < micro))
        def _():
            forward(t)

        @pl.when((mw >= 0) & (mw < micro))
        def _():
            by_weights(mw)

        return carry

    lax.fori_loop(0, micro + lead + lag, step, 0)

    for j in range(3):
        s_back(micro - 1, j).wait()

    out = [pltpu.make_async_copy(s_in.at[j], o, o_sem.at[j]) for j, o in enumerate((og, ou, od))]
    for j in range(3):
        s_in[j] = acc[j].astype(BF)
        out[j].start()

    @pl.when(me < last)
    def _():
        for m in (micro - 2, micro - 1):
            for p in range(PARTS):
                onward(m, p).wait_send()

    @pl.when(me > 0)
    def _():
        for m in (micro - 2, micro - 1):
            for p in range(PARTS):
                back_again(m, p).wait_send()

    for copy in out:
        copy.wait()


def solution(mesh):
    stages = mesh.shape["pp"]

    def step(x, dy, wg, wu, wd):
        micro, tokens, d = x.shape
        ff = wg.shape[2]
        vmem, dma = pltpu.VMEM, pltpu.SemaphoreType.DMA
        wide = jax.ShapeDtypeStruct((d, ff), BF)
        og, ou, od, _, _ = pl.pallas_call(
            functools.partial(kernel, stages),
            out_shape=(wide, wide, wide,
                       jax.ShapeDtypeStruct((micro, 2, tokens, ff), F32), jax.ShapeDtypeStruct((micro, 3, tokens, ff), BF)),
            in_specs=[pl.BlockSpec(memory_space=pl.ANY)] * 5,
            out_specs=[pl.BlockSpec(memory_space=pl.ANY)] * 5,
            scratch_shapes=[
                vmem((micro, tokens, d), BF), vmem((micro, tokens, d), BF),
                vmem((d, ff), BF), vmem((d, ff), BF), vmem((ff, d), BF),
                vmem((3, d, ff), F32),
                vmem((2, tokens, ff), F32), vmem((2, tokens, ff), F32),
                vmem((3, tokens, ff), BF), vmem((3, tokens, ff), BF), vmem((2, tokens // PARTS, ff), BF), vmem((VIA_SLOTS, tokens // PARTS, d), BF),
                vmem((2, tokens, d), BF), vmem((2, tokens, d), BF),
                vmem((d, tokens), BF), vmem((d, tokens), BF),
                dma((micro, PARTS)), dma((micro, PARTS)), dma((2, PARTS)), dma((2, PARTS)),
                dma((3,)), dma((PARTS,)), dma((PARTS,)), dma((PARTS,)), dma((3,)), dma((3,)), dma((VIA_SLOTS,)), dma,
            ],
            compiler_params=pltpu.CompilerParams(collective_id=0, has_side_effects=True, vmem_limit_bytes=67043328),
            name="pipeline",
        )(x, dy, wg[0], wu[0], wd[0])
        return og[None], ou[None], od.T[None]

    return jax.shard_map(
        step,
        mesh=mesh,
        in_specs=(P("rep", None, None),) * 2 + (P("pp", None, None),) * 3,
        out_specs=(P(("rep", "pp"), None, None),) * 3,
        check_vma=False,
    )
```

```python
import functools

import jax
import jax.numpy as jnp
from jax import lax
from jax.experimental import pallas as pl
from jax.experimental.pallas import tpu as pltpu
from jax.sharding import PartitionSpec as P

BF, F32 = jnp.bfloat16, jnp.float32
LEAD = (15, 13, 11, 10, 6, 5, 2, 0)
LAG = (2, 2, 4, 5, 9, 10, 10, 4)
VIA = range(3, 13)
VIA_SLOTS = 6
TILE = 256
PARTS = 2
NN = (((1,), (0,)), ((), ()))
NT = (((1,), (1,)), ((), ()))


def dot(a, b, dims=NN):
    return lax.dot_general(a, b, dims, preferred_element_type=F32)


def scaled(h):
    wide = h.astype(F32)
    return wide, lax.rsqrt(jnp.mean(wide * wide, -1, keepdims=True) + 1e-6)


def tiles(ff):
    return [pl.ds(n, TILE) for n in range(0, ff, TILE)]


def pick(me, values):
    out = jnp.int32(values[0])
    for i in range(1, len(values)):
        out = jnp.where(me == i, jnp.int32(values[i]), out)
    return out


def kernel(stages, x, dy, wg_in, wu_in, wd_in, og, ou, od, gu_all, s_all, *scratch):
    (hb, db, wg, wu, wd, acc, gu, gu_in, s_out, s_in, hid, via, ys, dhs, at, dyt,
     h_sem, d_sem, y_sent, dh_sent, w_sem, gu_sem, gu_in_sem, s_sem, s_in_sem, o_sem, via_sem, via_sent) = scratch
    micro, tokens, _ = hb.shape
    ff = wg.shape[1]
    rows = tokens // PARTS
    last = stages - 1
    me = lax.axis_index("pp")
    lead, lag = pick(me, LEAD), pick(me, LAG)
    parts = [pl.ds(p * rows, rows) for p in range(PARTS)]

    weights = [pltpu.make_async_copy(a, b, w_sem.at[j]) for j, (a, b) in enumerate(((wg_in, wg), (wu_in, wu), (wd_in, wd)))]
    for copy in weights:
        copy.start()

    @pl.when(me == 0)
    def _():
        for m in range(micro):
            for p, r in enumerate(parts):
                pltpu.make_async_copy(x.at[m, r], hb.at[m, r], h_sem.at[m, p]).start()

    @pl.when(me == last)
    def _():
        for m in range(micro):
            for p, r in enumerate(parts):
                pltpu.make_async_copy(dy.at[m, r], db.at[m, r], d_sem.at[m, p]).start()

    low, high = stages // 2 - 1, stages // 2
    peers = [(i, i + 1) for i in range(last)] + [(a, b) for a in (0, last) for b in (low, high)]
    barrier = pltpu.get_barrier_semaphore()
    for a, b in peers:
        for one, other in ((a, b), (b, a)):
            @pl.when(me == one)
            def _():
                pl.semaphore_signal(barrier, inc=1, device_id={"pp": other}, device_id_type=pl.DeviceIdType.MESH)

    acc[...] = jnp.zeros_like(acc)

    pl.semaphore_wait(barrier, pick(me, [sum(i in pair for pair in peers) for i in range(stages)]))

    for copy in weights:
        copy.wait()

    def onward(m, p):
        r = parts[p]
        return pltpu.make_async_remote_copy(
            src_ref=ys.at[m % 2, r], dst_ref=hb.at[m, r], send_sem=y_sent.at[m % 2, p], recv_sem=h_sem.at[m, p],
            device_id={"pp": me + 1}, device_id_type=pl.DeviceIdType.MESH)

    def back_again(m, p):
        r = parts[p]
        return pltpu.make_async_remote_copy(
            src_ref=dhs.at[m % 2, r], dst_ref=db.at[m, r], send_sem=dh_sent.at[m % 2, p], recv_sem=d_sem.at[m, p],
            device_id={"pp": me - 1}, device_id_type=pl.DeviceIdType.MESH)

    def remote(src, dst, sent, came, device):
        return pltpu.make_async_remote_copy(src_ref=src, dst_ref=dst, send_sem=sent, recv_sem=came,
                                            device_id={"pp": device}, device_id_type=pl.DeviceIdType.MESH)

    half = PARTS - 1

    def goes_via(m):
        return (m >= VIA.start) & (m < VIA.stop)

    def onward_via(m):
        return remote(ys.at[m % 2, parts[half]], via.at[m % VIA_SLOTS], y_sent.at[m % 2, half], via_sem.at[m % VIA_SLOTS], 0)

    def back_via(m):
        return remote(dhs.at[m % 2, parts[half]], via.at[m % VIA_SLOTS], dh_sent.at[m % 2, half], via_sem.at[m % VIA_SLOTS], last)

    def pass_onward(m):
        return remote(via.at[m % VIA_SLOTS], hb.at[m, parts[half]], via_sent, h_sem.at[m, half], high)

    def pass_back(m):
        return remote(via.at[m % VIA_SLOTS], db.at[m, parts[half]], via_sent, d_sem.at[m, half], low)

    def send(direct, indirect, m, p, at_stage):
        if p < half:
            direct(m, p).start()
            return
        other_way = (me == at_stage) & goes_via(m)

        @pl.when(other_way)
        def _():
            indirect(m).start()

        @pl.when(jnp.logical_not(other_way))
        def _():
            direct(m, p).start()

    def h_came(m, p):
        r = parts[p]
        return pltpu.make_async_copy(x.at[m, r], hb.at[m, r], h_sem.at[m, p])

    def d_came(m, p):
        r = parts[p]
        return pltpu.make_async_copy(dy.at[m, r], db.at[m, r], d_sem.at[m, p])

    def gu_out(m, p):
        return pltpu.make_async_copy(gu.at[:, parts[p]], gu_all.at[m, :, parts[p]], gu_sem.at[p])

    def gu_back(m, p):
        return pltpu.make_async_copy(gu_all.at[m, :, parts[p]], gu_in.at[:, parts[p]], gu_in_sem.at[p])

    def s_save(m, p):
        return pltpu.make_async_copy(s_out.at[:, parts[p]], s_all.at[m, :, parts[p]], s_sem.at[p])

    def s_back(m, j):
        return pltpu.make_async_copy(s_all.at[m, j], s_in.at[j], s_in_sem.at[j])

    def forward(m):
        @pl.when(m >= 1)
        def _():
            for p in range(PARTS):
                gu_out(m - 1, p).wait()

        @pl.when(m >= 2)
        def _():
            for p in range(PARTS):
                onward(m - 2, p).wait_send()

        for p, r in enumerate(parts):
            h_came(m, p).wait()
            h = hb[m, r, :]
            wide, scale = scaled(h)
            a = (wide * scale).astype(BF)
            for n in tiles(ff):
                g, u = dot(a, wg[:, n]), dot(a, wu[:, n])
                gu[0, r, n] = g
                gu[1, r, n] = u
                hid[p % 2, :, n] = (g * jax.nn.sigmoid(g) * u).astype(BF)
            y = dot(hid[p % 2], wd[...]).astype(BF)
            ys[m % 2, r, :] = h + y
            send(onward, onward_via, m, p, low)
            gu_out(m, p).start()

    def by_hidden(d, g, u, r, n):
        by_hid = dot(d, wd[n, :], NT).astype(BF).astype(F32)
        s = jax.nn.sigmoid(g)
        sg = g * s
        s_out[2, r, n] = (sg * u).astype(BF)
        s_out[1, r, n] = (sg * by_hid).astype(BF)
        s_out[0, r, n] = (by_hid * u * (s + sg * (1.0 - s))).astype(BF)

    def by_input(m, r, d):
        da = dot(s_out[0, r, :], wg[...], NT).astype(BF) + dot(s_out[1, r, :], wu[...], NT).astype(BF)
        wide, scale = scaled(hb[m, r, :])
        da = da.astype(F32)
        c = jnp.sum(wide * da, -1, keepdims=True) * (scale * scale * scale) * (1.0 / hb.shape[2])
        dhs[m % 2, r, :] = d + (da * scale - wide * c).astype(BF)

    def backward_part(m, p, first, final):
        r = parts[p]
        d_came(m, p).wait()
        d = db[m, r, :]
        if final:
            h_came(m, p).wait()
            wide, scale = scaled(hb[m, r, :])
            a = (wide * scale).astype(BF)
            for n in tiles(ff):
                by_hidden(d, dot(a, wg[:, n]), dot(a, wu[:, n]), r, n)
        else:
            gu_back(m, p).wait()
            for n in tiles(ff):
                by_hidden(d, gu_in[0, r, n], gu_in[1, r, n], r, n)
        if not first:
            by_input(m, r, d)
            send(back_again, back_via, m, p, high)
        s_save(m, p).start()
        if not final:
            gu_back(jnp.minimum(m + 1, micro - 1), p).start()

    def backward(m):
        for first, final, here in ((True, False, me == 0), (False, False, (me > 0) & (me < last)), (False, True, me == last)):
            @pl.when(here)
            def _():
                @pl.when(m >= 1)
                def _():
                    for p in range(PARTS):
                        s_save(m - 1, p).wait()

                if not first:
                    @pl.when(m >= 2)
                    def _():
                        for p in range(PARTS):
                            back_again(m - 2, p).wait_send()

                for p in range(PARTS):
                    backward_part(m, p, first, final)

    def by_weights(m):
        for j in range(3):
            s_back(m, j).wait()
        dyt[...] = db[m].T
        wide, scale = scaled(hb[m])
        at[...] = (wide * scale).astype(BF).T
        for j, left in ((2, dyt), (0, at), (1, at)):
            for n in tiles(ff):
                acc[j, :, n] += dot(left[...], s_in[j, :, n]).astype(BF).astype(F32)
        for j in range(3):
            s_back(jnp.minimum(m + 1, micro - 1), j).start()

    def step(t, carry):
        mb, mw = t - lead, t - lead - lag
        passed = t - VIA_SLOTS

        @pl.when((me == 0) & goes_via(passed))
        def _():
            pass_onward(passed).wait_send()

        @pl.when((me == last) & goes_via(passed))
        def _():
            pass_back(passed).wait_send()

        @pl.when((me == 0) & goes_via(passed + 1))
        def _():
            onward_via(passed + 1).wait_recv()
            pass_onward(passed + 1).start()

        @pl.when((me == last) & goes_via(passed + 1))
        def _():
            back_via(passed + 1).wait_recv()
            pass_back(passed + 1).start()

        @pl.when((me < last) & (t == micro))
        def _():
            for p in range(PARTS):
                gu_out(micro - 1, p).wait()

        @pl.when(mb == micro)
        def _():
            for p in range(PARTS):
                s_save(micro - 1, p).wait()

        @pl.when((me < last) & (mb == micro))
        def _():
            for p in range(PARTS):
                gu_back(micro - 1, p).wait()

        @pl.when((me < last) & (mb == 0))
        def _():
            for p in range(PARTS):
                gu_back(0, p).start()

        @pl.when(mw == 0)
        def _():
            for j in range(3):
                s_back(0, j).start()

        @pl.when((me < last) & (t < micro))
        def _():
            forward(t)

        @pl.when((mb >= 0) & (mb < micro))
        def _():
            backward(mb)

        @pl.when((mw >= 0) & (mw < micro))
        def _():
            by_weights(mw)

        return carry

    lax.fori_loop(0, micro + lead + lag, step, 0)

    for j in range(3):
        s_back(micro - 1, j).wait()

    out = [pltpu.make_async_copy(s_in.at[j], o, o_sem.at[j]) for j, o in enumerate((og, ou, od))]
    for j in range(3):
        s_in[j] = acc[j].astype(BF)
        out[j].start()

    @pl.when(me < last)
    def _():
        for m in (micro - 2, micro - 1):
            for p in range(PARTS):
                onward(m, p).wait_send()

    @pl.when(me > 0)
    def _():
        for m in (micro - 2, micro - 1):
            for p in range(PARTS):
                back_again(m, p).wait_send()

    for copy in out:
        copy.wait()


def solution(mesh):
    stages = mesh.shape["pp"]

    def step(x, dy, wg, wu, wd):
        micro, tokens, d = x.shape
        ff = wg.shape[2]
        vmem, dma = pltpu.VMEM, pltpu.SemaphoreType.DMA
        wide = jax.ShapeDtypeStruct((d, ff), BF)
        og, ou, od, _, _ = pl.pallas_call(
            functools.partial(kernel, stages),
            out_shape=(wide, wide, wide,
                       jax.ShapeDtypeStruct((micro, 2, tokens, ff), F32), jax.ShapeDtypeStruct((micro, 3, tokens, ff), BF)),
            in_specs=[pl.BlockSpec(memory_space=pl.ANY)] * 5,
            out_specs=[pl.BlockSpec(memory_space=pl.ANY)] * 5,
            scratch_shapes=[
                vmem((micro, tokens, d), BF), vmem((micro, tokens, d), BF),
                vmem((d, ff), BF), vmem((d, ff), BF), vmem((ff, d), BF),
                vmem((3, d, ff), F32),
                vmem((2, tokens, ff), F32), vmem((2, tokens, ff), F32),
                vmem((3, tokens, ff), BF), vmem((3, tokens, ff), BF), vmem((2, tokens // PARTS, ff), BF), vmem((VIA_SLOTS, tokens // PARTS, d), BF),
                vmem((2, tokens, d), BF), vmem((2, tokens, d), BF),
                vmem((d, tokens), BF), vmem((d, tokens), BF),
                dma((micro, PARTS)), dma((micro, PARTS)), dma((2, PARTS)), dma((2, PARTS)),
                dma((3,)), dma((PARTS,)), dma((PARTS,)), dma((PARTS,)), dma((3,)), dma((3,)), dma((VIA_SLOTS,)), dma,
            ],
            compiler_params=pltpu.CompilerParams(collective_id=0, has_side_effects=True, vmem_limit_bytes=67043328),
            name="pipeline",
        )(x, dy, wg[0], wu[0], wd[0])
        return og[None], ou[None], od.T[None]

    return jax.shard_map(
        step,
        mesh=mesh,
        in_specs=(P("rep", None, None),) * 2 + (P("pp", None, None),) * 3,
        out_specs=(P(("rep", "pp"), None, None),) * 3,
        check_vma=False,
    )
```
